32 devices in a mesh: section: 2 (over y), rep: 4 (over z), sub: 4 (over x, core).
Axes of the slice: x: 2, y: 2, z: 4, core: 2. Of those that a mesh axis runs over, the one named last changes fastest.
Arguments:
- token_ids: int32 [8, 512], P(None, ('rep', 'sub')), may hold values from 0 to 255
- target_ids: int32 [8, 512], P(None, ('rep', 'sub')), may hold values from 0 to 255
- embedding: bfloat16 [256, 2048], P(('rep', 'sub')), may hold values from -3 to 3
- section_weight: bfloat16 [2, 2048, 2048], P('section', ('rep', 'sub')), may hold values from -0.125 to 0.125
- section_gain: float32 [2, 2048], P('section'), may hold values from 0.1 to 1.9
- final_gain: float32 [2048], replicated, may hold values from 0.5 to 1.5
Outputs:
- weight_grad: float32 [2, 2048, 2048], P('section', ('rep', 'sub'))
- gain_grad: float32 [2, 2048], P('section')
- embed_grad: float32 [256, 2048], P(('section', 'rep', 'sub'))
- final_grad: float32 [2048], replicated
The draws below stay inside these ranges and needn't reach their ends.
All inputs are finite; a program needn't handle non-finite values.
Results may differ from the reference program's by a relative error of at most 0.024.
Values may be sent and summed in bfloat16 or wider, within the bound.
A program may use at most 64 MiB of HBM per device.

```python
import math
import jax
import jax.numpy as jnp
import numpy as np
from jax import lax

D = 2048
VOCAB = 256
MICRO = 8
SECTIONS = 2
TOKENS = 512
N_SECTION = 2


def set_ends(entries, key, low, largest):
    index_at = [jax.random.randint(jax.random.fold_in(key, axis), (), 0, length) for axis, length in enumerate(entries.shape)]
    main_axis = entries.shape.index(max(entries.shape))
    neighbour = index_at[:main_axis] + [(index_at[main_axis] + 1) % entries.shape[main_axis]] + index_at[main_axis + 1:]
    return entries.at[tuple(index_at)].set(low).at[tuple(neighbour)].set(largest)


def block_levels(key, extent, pieces, low, top_value):
    level = 1.0
    for axis_at, shards_of in pieces:
        draws = jax.random.uniform(jax.random.fold_in(jax.random.fold_in(key, 6), axis_at), (shards_of,), jnp.float32, low / len(pieces), top_value / len(pieces))
        level = level * jnp.repeat(jnp.exp(draws), extent[axis_at] // shards_of).reshape((-1,) + (1,) * (len(extent) - 1 - axis_at))
    return level


def cumulative_ranks(amount, slope):
    portions = [(1 << 20) // math.isqrt(grade ** slope) + 1 for grade in range(1, amount + 1)]
    width = 1 + sum(portions) // (1 << 30)
    return np.cumsum(np.array([max(1, weight // width) for weight in portions]))


def ranked(own_key, extent, count, lean):
    grid = cumulative_ranks(count, lean)
    pick = jax.random.randint(jax.random.fold_in(own_key, 1), extent, 0, int(grid[count - 1]))
    rank = jnp.searchsorted(jnp.asarray(grid, jnp.int32), pick, side="right")
    return jax.random.permutation(jax.random.fold_in(own_key, 2), count)[rank].astype(jnp.int32)


def centred(rng, shape, spread, most, split=(), kind=jnp.bfloat16):
    drawn = spread * jax.random.normal(rng, shape, jnp.float32)
    if split:
        drawn = drawn * block_levels(rng, shape, split, -0.22, 0.18)
    return jnp.clip(drawn, -most, most).astype(kind)


def setup_inputs(seed: int = 0) -> dict:
    key_list = jax.random.split(jax.random.key(seed), 7)
    return {
        "token_ids": set_ends(ranked(key_list[0], (MICRO, TOKENS), VOCAB, 2), jax.random.fold_in(key_list[0], 3), 0, VOCAB - 1).astype(jnp.int32),
        "target_ids": set_ends(ranked(key_list[1], (MICRO, TOKENS), VOCAB, 1), jax.random.fold_in(key_list[1], 3), 0, VOCAB - 1).astype(jnp.int32),
        "embedding": centred(key_list[2], (VOCAB, D), 0.25, 3.0, ((0, 16),)),
        "section_weight": centred(key_list[3], (SECTIONS, D, D), D ** -0.5, 0.125, ((0, 2), (1, 16))),
        "section_gain": jnp.clip(1.0 + 0.18 * jax.random.normal(key_list[4], (SECTIONS, D), jnp.float32), 0.1, 1.9),
        "final_gain": jnp.clip(1.0 + 0.1 * jax.random.normal(key_list[5], (D,), jnp.float32), 0.5, 1.5),
    }


epsilon = 1e-06
gelu_coef = 0.7978845608028654
cube_coef = 0.044715

def gelu(pre_act):
    return 0.5 * pre_act * (1.0 + jnp.tanh(gelu_coef * (pre_act + cube_coef * pre_act * pre_act * pre_act)))

def gelu_slope(pre_act):
    inside = gelu_coef * (pre_act + cube_coef * pre_act * pre_act * pre_act)
    tangent = jnp.tanh(inside)
    return 0.5 * (1.0 + tangent) + 0.5 * pre_act * (1.0 - tangent * tangent) * gelu_coef * (1.0 + 3.0 * cube_coef * pre_act * pre_act)

def normalize(residual, gain_row):
    values = residual.astype(jnp.float32)
    scale_inv = lax.rsqrt(lax.optimization_barrier(jnp.mean(values * values, axis=-1, keepdims=True)) + epsilon)
    normed = values * scale_inv
    return (normed, scale_inv, (normed * gain_row).astype(jnp.bfloat16))

def norm_back(grad_norm, normed, scale_inv, gain_row):
    grad_unit = grad_norm * gain_row
    grad_in = scale_inv * (grad_unit - normed * lax.optimization_barrier(jnp.mean(grad_unit * normed, axis=-1, keepdims=True)))
    return (grad_in, lax.optimization_barrier(jnp.sum(grad_norm * normed, axis=0)))

def reference(token_ids, target_ids, embedding, section_weight, section_gain, final_gain):
    vocab_iota = jnp.arange(VOCAB, dtype=jnp.int32)
    onehot_in = (token_ids.reshape(-1)[:, None] == vocab_iota[None, :]).astype(jnp.bfloat16)
    residual = jnp.dot(onehot_in, embedding, preferred_element_type=jnp.float32).astype(jnp.bfloat16)
    saved = []
    for layer_index in range(N_SECTION):
        normed, scale_inv, rounded = normalize(residual, section_gain[layer_index])
        pre_act = jnp.dot(rounded, section_weight[layer_index], preferred_element_type=jnp.float32)
        saved.append((residual, rounded, pre_act))
        residual = (residual.astype(jnp.float32) + gelu(pre_act)).astype(jnp.bfloat16)
    normed, scale_inv, final_rows = normalize(residual, final_gain)
    logit_scale = float(D) ** (-0.5)
    contract_last = (((1,), (1,)), ((), ()))
    contract_first = (((0,), (0,)), ((), ()))
    logits = lax.dot_general(final_rows, embedding, contract_last, preferred_element_type=jnp.float32) * logit_scale
    exp_logit = jnp.exp(logits)
    probability = exp_logit / lax.optimization_barrier(jnp.sum(exp_logit, axis=-1, keepdims=True))
    onehot_out = (target_ids.reshape(-1)[:, None] == vocab_iota[None, :]).astype(jnp.float32)
    grad_logit = ((probability - onehot_out) * logit_scale).astype(jnp.bfloat16)
    embed_head = lax.dot_general(grad_logit, final_rows, contract_first, preferred_element_type=jnp.float32)
    grad_final = jnp.dot(grad_logit, embedding, preferred_element_type=jnp.float32)
    grad_in, final_grad = norm_back(grad_final, normed, scale_inv, final_gain)
    grad_residual = grad_in.astype(jnp.bfloat16)
    weight_list = []
    gain_list = []
    for layer_index in reversed(range(N_SECTION)):
        residual_in, rounded, pre_act = saved[layer_index]
        grad_float = grad_residual.astype(jnp.float32)
        grad_pre = (grad_float * gelu_slope(pre_act)).astype(jnp.bfloat16)
        weight_list.append(lax.dot_general(rounded, grad_pre, contract_first, preferred_element_type=jnp.float32))
        grad_norm = lax.dot_general(grad_pre, section_weight[layer_index], contract_last, preferred_element_type=jnp.float32)
        normed, scale_inv, rounded_again = normalize(residual_in, section_gain[layer_index])
        grad_in, gain_part = norm_back(grad_norm, normed, scale_inv, section_gain[layer_index])
        gain_list.append(gain_part)
        grad_residual = (grad_float + grad_in).astype(jnp.bfloat16)
    embed_in = lax.dot_general(onehot_in, grad_residual, contract_first, preferred_element_type=jnp.float32)
    weight_grad = jnp.stack(weight_list[::-1])
    gain_grad = jnp.stack(gain_list[::-1])
    return (weight_grad, gain_grad, embed_in + embed_head, final_grad)
```

```python
import jax
import jax.numpy as jnp
from jax import lax
from jax.sharding import PartitionSpec as P

epsilon = 1e-06
gelu_coef = 0.7978845608028654
cube_coef = 0.044715


def passed_along(value, axis, steps):
    count = lax.axis_size(axis)
    initial, last = (max(0, -steps), min(count, count - steps))
    return lax.ppermute(value, axis, [(source, source + steps) for source in range(initial, last)])


def gelu(pre_act):
    return (
        0.5
        * pre_act
        * (1.0 + jnp.tanh(gelu_coef * (pre_act + cube_coef * pre_act * pre_act * pre_act)))
    )


def gelu_slope(pre_act):
    inside = gelu_coef * (pre_act + cube_coef * pre_act * pre_act * pre_act)
    tangent = jnp.tanh(inside)
    return 0.5 * (1.0 + tangent) + 0.5 * pre_act * (1.0 - tangent * tangent) * gelu_coef * (
        1.0 + 3.0 * cube_coef * pre_act * pre_act
    )


def normalize(residual, gain_row):
    values = residual.astype(jnp.float32)
    scale_inv = lax.rsqrt(jnp.mean(values * values, axis=-1, keepdims=True) + epsilon)
    normed = values * scale_inv
    return (normed, scale_inv, (normed * gain_row).astype(jnp.bfloat16))


def norm_back(grad_norm, normed, scale_inv, gain_row):
    grad_unit = grad_norm * gain_row
    grad_in = scale_inv * (
        grad_unit - normed * jnp.mean(grad_unit * normed, axis=-1, keepdims=True)
    )
    return (grad_in, jnp.sum(grad_norm * normed, axis=0))


def pick_slot(buffer, slot_index):
    return lax.dynamic_index_in_dim(buffer, slot_index, 0, keepdims=False)


def place_slot(buffer, update, slot_index):
    return lax.dynamic_update_index_in_dim(buffer, update, slot_index, 0)


def pipeline_body(token_ids, target_ids, embedding, section_weight, section_gain, final_gain):
    sections = lax.axis_size("section")
    position = lax.axis_index("section")
    micro_count = token_ids.shape[0]
    row_count = token_ids.shape[1]
    features = embedding.shape[1]
    group_size = lax.axis_size(("rep", "sub"))
    vocab_rows = embedding.shape[0] * group_size
    tick_count = micro_count + sections - 1
    contract_last = (((1,), (1,)), ((), ()))
    contract_first = (((0,), (0,)), ((), ()))
    vocab_table = lax.all_gather(embedding, ("rep", "sub"), axis=0, tiled=True)
    weight = lax.all_gather(section_weight, ("rep", "sub"), axis=1, tiled=True)[0]
    gain_row = section_gain[0]
    is_first = position == 0
    is_last = position == sections - 1
    vocab_iota = jnp.arange(vocab_rows, dtype=jnp.int32)
    onehot_in = (token_ids.reshape(-1)[:, None] == vocab_iota[None, :]).astype(jnp.bfloat16)
    embedded = jnp.dot(onehot_in, vocab_table, preferred_element_type=jnp.float32).astype(
        jnp.bfloat16
    )
    embedded = embedded.reshape(micro_count, row_count, features)
    empty_rows = jnp.zeros((row_count, features), jnp.bfloat16)
    zeros_stash = jnp.zeros((micro_count, row_count, features), jnp.bfloat16)
    zeros_pre = jnp.zeros((micro_count, row_count, features), jnp.float32)

    def forward_tick(carried, tick_index):
        arrived = carried[0]
        buffers = carried[1:]
        offset = tick_index - position
        active = (offset >= 0) & (offset < micro_count)
        slot_index = jnp.clip(offset, 0, micro_count - 1)
        residual = jnp.where(is_first, pick_slot(embedded, slot_index), arrived)

        def forward_compute(kept_activations):
            input_list, rounded_list, preactivation_list, output_list = kept_activations
            normed, scale_inv, rounded = normalize(residual, gain_row)
            pre_act = jnp.dot(rounded, weight, preferred_element_type=jnp.float32)
            returned_value = (residual.astype(jnp.float32) + gelu(pre_act)).astype(jnp.bfloat16)
            kept_activations = (
                place_slot(input_list, residual, slot_index),
                place_slot(rounded_list, rounded, slot_index),
                place_slot(preactivation_list, pre_act, slot_index),
                place_slot(output_list, returned_value, slot_index),
            )
            return (kept_activations, returned_value)

        def forward_bypass(kept_activations):
            return (kept_activations, empty_rows)

        buffers, returned_value = lax.cond(active, forward_compute, forward_bypass, buffers)
        arrived = passed_along(returned_value, "section", 1)
        return ((arrived,) + buffers, None)

    start_state = (empty_rows, zeros_stash, zeros_stash, zeros_pre, zeros_stash)
    final_state, unused_out = lax.scan(
        forward_tick, start_state, jnp.arange(tick_count, dtype=jnp.int32)
    )
    input_list, rounded_list, preactivation_list, output_list = final_state[1:]
    logit_scale = float(features) ** (-0.5)

    def head(finals):
        normed, scale_inv, final_rows = normalize(finals, final_gain)
        logits = (
            lax.dot_general(
                final_rows, vocab_table, contract_last, preferred_element_type=jnp.float32
            )
            * logit_scale
        )
        exp_logit = jnp.exp(logits)
        probability = exp_logit / jnp.sum(exp_logit, axis=-1, keepdims=True)
        onehot_out = (target_ids.reshape(-1)[:, None] == vocab_iota[None, :]).astype(jnp.float32)
        grad_logit = ((probability - onehot_out) * logit_scale).astype(jnp.bfloat16)
        embed_head = lax.dot_general(
            grad_logit, final_rows, contract_first, preferred_element_type=jnp.float32
        )
        grad_final = jnp.dot(grad_logit, vocab_table, preferred_element_type=jnp.float32)
        grad_in, final_part = norm_back(grad_final, normed, scale_inv, final_gain)
        grad_top = grad_in.astype(jnp.bfloat16).reshape(micro_count, row_count, features)
        return (embed_head, grad_top, final_part)

    def no_head(finals):
        return (
            jnp.zeros((vocab_rows, features), jnp.float32),
            zeros_stash,
            jnp.zeros((features,), jnp.float32),
        )

    embed_head, grad_top, final_part = lax.cond(
        is_last, head, no_head, output_list.reshape(-1, features)
    )

    def backward_tick(carried, tick_index):
        arrived = carried[0]
        buffers = carried[1:]
        offset = tick_index - (sections - 1 - position)
        active = (offset >= 0) & (offset < micro_count)
        slot_index = jnp.clip(offset, 0, micro_count - 1)
        grad_out = jnp.where(is_last, pick_slot(grad_top, slot_index), arrived)

        def backward_compute(kept_activations):
            preactivation_gradients, first_row_gradients, gain_accumulated = kept_activations
            grad_float = grad_out.astype(jnp.float32)
            grad_pre = (grad_float * gelu_slope(pick_slot(preactivation_list, slot_index))).astype(
                jnp.bfloat16
            )
            grad_norm = lax.dot_general(
                grad_pre, weight, contract_last, preferred_element_type=jnp.float32
            )
            normed, scale_inv, rounded = normalize(pick_slot(input_list, slot_index), gain_row)
            grad_in, gain_part = norm_back(grad_norm, normed, scale_inv, gain_row)
            sent_output = (grad_float + grad_in).astype(jnp.bfloat16)
            kept_activations = (
                place_slot(preactivation_gradients, grad_pre, slot_index),
                place_slot(first_row_gradients, sent_output, slot_index),
                gain_accumulated + gain_part,
            )
            return (kept_activations, sent_output)

        def backward_bypass(kept_activations):
            return (kept_activations, empty_rows)

        buffers, sent_output = lax.cond(active, backward_compute, backward_bypass, buffers)
        arrived = passed_along(sent_output, "section", -1)
        return ((arrived,) + buffers, None)

    back_state = (empty_rows, zeros_stash, zeros_stash, jnp.zeros((features,), jnp.float32))
    back_final, unused_back = lax.scan(
        backward_tick, back_state, jnp.arange(tick_count, dtype=jnp.int32)
    )
    preactivation_gradients, first_row_gradients, gain_accumulated = back_final[1:]
    pres_flat = preactivation_gradients.reshape(-1, features)
    rounded_flat = rounded_list.reshape(-1, features)
    weight_part = lax.psum_scatter(
        lax.dot_general(
            rounded_flat, pres_flat, contract_first, preferred_element_type=jnp.float32
        ).astype(jnp.bfloat16),
        ("rep", "sub"),
        scatter_dimension=0,
        tiled=True,
    ).astype(jnp.float32)
    gain_total = lax.psum(gain_accumulated, ("rep", "sub"))
    final_total = lax.psum(final_part, ("section", "rep", "sub"))
    embed_in = lax.dot_general(
        onehot_in,
        first_row_gradients.reshape(-1, features),
        contract_first,
        preferred_element_type=jnp.float32,
    )
    contribution = jnp.where(is_first, embed_in, 0.0) + embed_head
    embed_total = lax.psum_scatter(
        contribution, ("section", "rep", "sub"), scatter_dimension=0, tiled=True
    )
    return (weight_part[None], gain_total[None], embed_total, final_total)


def fits_replicated(mesh, weight_shape):
    layers, rows, columns = weight_shape
    return layers * rows * columns * 2 <= 16 * 1024 * 1024


def replicated_body(token_ids, target_ids, embedding, section_weight, section_gain, final_gain):
    axes = ("section", "rep", "sub")
    sections = lax.axis_size("section")
    position = lax.axis_index("section")
    features = embedding.shape[1]
    vocab_rows = embedding.shape[0] * lax.axis_size(("rep", "sub"))
    token_count = token_ids.size // sections
    contract_last = (((1,), (1,)), ((), ()))
    contract_first = (((0,), (0,)), ((), ()))
    vocab_table = lax.all_gather(embedding, ("rep", "sub"), axis=0, tiled=True)
    weights = lax.all_gather(section_weight[0], axes, axis=0, tiled=True)
    weights = weights.reshape(sections, features, features)
    gains = lax.all_gather(section_gain, "section", axis=0, tiled=True)
    my_tokens = lax.dynamic_slice_in_dim(token_ids.reshape(-1), position * token_count, token_count)
    my_targets = lax.dynamic_slice_in_dim(target_ids.reshape(-1), position * token_count, token_count)
    vocab_iota = jnp.arange(vocab_rows, dtype=jnp.int32)
    onehot_in = (my_tokens[:, None] == vocab_iota[None, :]).astype(jnp.bfloat16)
    residual = jnp.dot(onehot_in, vocab_table, preferred_element_type=jnp.float32).astype(
        jnp.bfloat16
    )
    saved = []
    for layer in range(sections):
        normed, scale_inv, rounded = normalize(residual, gains[layer])
        pre_act = jnp.dot(rounded, weights[layer], preferred_element_type=jnp.float32)
        saved.append((normed, scale_inv, rounded, pre_act))
        residual = (residual.astype(jnp.float32) + gelu(pre_act)).astype(jnp.bfloat16)
    logit_scale = float(features) ** (-0.5)
    normed, scale_inv, final_rows = normalize(residual, final_gain)
    logits = (
        lax.dot_general(final_rows, vocab_table, contract_last, preferred_element_type=jnp.float32)
        * logit_scale
    )
    exp_logit = jnp.exp(logits)
    probability = exp_logit / jnp.sum(exp_logit, axis=-1, keepdims=True)
    onehot_out = (my_targets[:, None] == vocab_iota[None, :]).astype(jnp.float32)
    grad_logit = ((probability - onehot_out) * logit_scale).astype(jnp.bfloat16)
    embed_head = lax.dot_general(
        grad_logit, final_rows, contract_first, preferred_element_type=jnp.float32
    )
    grad_final = jnp.dot(grad_logit, vocab_table, preferred_element_type=jnp.float32)
    grad_in, final_part = norm_back(grad_final, normed, scale_inv, final_gain)
    grad_residual = grad_in.astype(jnp.bfloat16)
    weight_parts = []
    small_parts = [final_part]
    for layer in reversed(range(sections)):
        normed, scale_inv, rounded, pre_act = saved[layer]
        grad_float = grad_residual.astype(jnp.float32)
        grad_pre = (grad_float * gelu_slope(pre_act)).astype(jnp.bfloat16)
        weight_parts.append(
            lax.dot_general(
                rounded, grad_pre, contract_first, preferred_element_type=jnp.float32
            ).astype(jnp.bfloat16)
        )
        grad_norm = lax.dot_general(
            grad_pre, weights[layer], contract_last, preferred_element_type=jnp.float32
        )
        grad_in, gain_part = norm_back(grad_norm, normed, scale_inv, gains[layer])
        small_parts.append(gain_part)
        grad_residual = (grad_float + grad_in).astype(jnp.bfloat16)
    embed_part = embed_head + lax.dot_general(
        onehot_in, grad_residual, contract_first, preferred_element_type=jnp.float32
    )
    return finish(weight_parts[::-1], embed_part, jnp.stack(small_parts), axes, position, sections)


def finish(weight_parts, embed_part, small_part, axes, position, sections):
    weight_all = jnp.concatenate(weight_parts, axis=0)
    weight_total = lax.psum_scatter(weight_all, axes, scatter_dimension=0, tiled=True)
    embed_total = lax.psum_scatter(embed_part, axes, scatter_dimension=0, tiled=True)
    small_total = lax.psum(small_part, axes)
    gain_total = lax.dynamic_slice_in_dim(small_total, sections - position, 1, axis=0)
    return (weight_total.astype(jnp.float32)[None], gain_total, embed_total, small_total[0])


def solution(mesh):
    in_specs = (
        P(None, ("rep", "sub")),
        P(None, ("rep", "sub")),
        P(("rep", "sub"), None),
        P("section", ("rep", "sub"), None),
        P("section", None),
        P(),
    )
    out_specs = (
        P("section", ("rep", "sub"), None),
        P("section", None),
        P(("section", "rep", "sub"), None),
        P(),
    )

    def step(*arguments):
        tokens = arguments[0].size // (mesh.shape["rep"] * mesh.shape["sub"])
        replicated = fits_replicated(mesh, arguments[3].shape) and tokens % mesh.shape["section"] == 0
        chosen = replicated_body if replicated else pipeline_body
        return jax.shard_map(
            chosen, mesh=mesh, in_specs=in_specs, out_specs=out_specs, check_vma=False
        )(*arguments)

    return step
```

```python
import functools
import jax
import jax.numpy as jnp
from jax import lax
from jax.experimental import pallas as pl
from jax.experimental.pallas import tpu as pltpu
from jax.sharding import PartitionSpec as P

epsilon = 1e-06
gelu_coef = 0.7978845608028654
cube_coef = 0.044715


def passed_along(value, axis, steps):
    count = lax.axis_size(axis)
    initial, last = (max(0, -steps), min(count, count - steps))
    return lax.ppermute(value, axis, [(source, source + steps) for source in range(initial, last)])


def gelu(pre_act):
    return (
        0.5
        * pre_act
        * (1.0 + jnp.tanh(gelu_coef * (pre_act + cube_coef * pre_act * pre_act * pre_act)))
    )


def gelu_slope(pre_act):
    inside = gelu_coef * (pre_act + cube_coef * pre_act * pre_act * pre_act)
    tangent = jnp.tanh(inside)
    return 0.5 * (1.0 + tangent) + 0.5 * pre_act * (1.0 - tangent * tangent) * gelu_coef * (
        1.0 + 3.0 * cube_coef * pre_act * pre_act
    )


def normalize(residual, gain_row):
    values = residual.astype(jnp.float32)
    scale_inv = lax.rsqrt(jnp.mean(values * values, axis=-1, keepdims=True) + epsilon)
    normed = values * scale_inv
    return (normed, scale_inv, (normed * gain_row).astype(jnp.bfloat16))


def norm_back(grad_norm, normed, scale_inv, gain_row):
    grad_unit = grad_norm * gain_row
    grad_in = scale_inv * (
        grad_unit - normed * jnp.mean(grad_unit * normed, axis=-1, keepdims=True)
    )
    return (grad_in, jnp.sum(grad_norm * normed, axis=0))


def pick_slot(buffer, slot_index):
    return lax.dynamic_index_in_dim(buffer, slot_index, 0, keepdims=False)


def place_slot(buffer, update, slot_index):
    return lax.dynamic_update_index_in_dim(buffer, update, slot_index, 0)


def pipeline_body(token_ids, target_ids, embedding, section_weight, section_gain, final_gain):
    sections = lax.axis_size("section")
    position = lax.axis_index("section")
    micro_count = token_ids.shape[0]
    row_count = token_ids.shape[1]
    features = embedding.shape[1]
    group_size = lax.axis_size(("rep", "sub"))
    vocab_rows = embedding.shape[0] * group_size
    tick_count = micro_count + sections - 1
    contract_last = (((1,), (1,)), ((), ()))
    contract_first = (((0,), (0,)), ((), ()))
    vocab_table = lax.all_gather(embedding, ("rep", "sub"), axis=0, tiled=True)
    weight = lax.all_gather(section_weight, ("rep", "sub"), axis=1, tiled=True)[0]
    gain_row = section_gain[0]
    is_first = position == 0
    is_last = position == sections - 1
    vocab_iota = jnp.arange(vocab_rows, dtype=jnp.int32)
    onehot_in = (token_ids.reshape(-1)[:, None] == vocab_iota[None, :]).astype(jnp.bfloat16)
    embedded = jnp.dot(onehot_in, vocab_table, preferred_element_type=jnp.float32).astype(
        jnp.bfloat16
    )
    embedded = embedded.reshape(micro_count, row_count, features)
    empty_rows = jnp.zeros((row_count, features), jnp.bfloat16)
    zeros_stash = jnp.zeros((micro_count, row_count, features), jnp.bfloat16)
    zeros_pre = jnp.zeros((micro_count, row_count, features), jnp.float32)

    def forward_tick(carried, tick_index):
        arrived = carried[0]
        buffers = carried[1:]
        offset = tick_index - position
        active = (offset >= 0) & (offset < micro_count)
        slot_index = jnp.clip(offset, 0, micro_count - 1)
        residual = jnp.where(is_first, pick_slot(embedded, slot_index), arrived)

        def forward_compute(kept_activations):
            input_list, rounded_list, preactivation_list, output_list = kept_activations
            normed, scale_inv, rounded = normalize(residual, gain_row)
            pre_act = jnp.dot(rounded, weight, preferred_element_type=jnp.float32)
            returned_value = (residual.astype(jnp.float32) + gelu(pre_act)).astype(jnp.bfloat16)
            kept_activations = (
                place_slot(input_list, residual, slot_index),
                place_slot(rounded_list, rounded, slot_index),
                place_slot(preactivation_list, pre_act, slot_index),
                place_slot(output_list, returned_value, slot_index),
            )
            return (kept_activations, returned_value)

        def forward_bypass(kept_activations):
            return (kept_activations, empty_rows)

        buffers, returned_value = lax.cond(active, forward_compute, forward_bypass, buffers)
        arrived = passed_along(returned_value, "section", 1)
        return ((arrived,) + buffers, None)

    start_state = (empty_rows, zeros_stash, zeros_stash, zeros_pre, zeros_stash)
    final_state, unused_out = lax.scan(
        forward_tick, start_state, jnp.arange(tick_count, dtype=jnp.int32)
    )
    input_list, rounded_list, preactivation_list, output_list = final_state[1:]
    logit_scale = float(features) ** (-0.5)

    def head(finals):
        normed, scale_inv, final_rows = normalize(finals, final_gain)
        logits = (
            lax.dot_general(
                final_rows, vocab_table, contract_last, preferred_element_type=jnp.float32
            )
            * logit_scale
        )
        exp_logit = jnp.exp(logits)
        probability = exp_logit / jnp.sum(exp_logit, axis=-1, keepdims=True)
        onehot_out = (target_ids.reshape(-1)[:, None] == vocab_iota[None, :]).astype(jnp.float32)
        grad_logit = ((probability - onehot_out) * logit_scale).astype(jnp.bfloat16)
        embed_head = lax.dot_general(
            grad_logit, final_rows, contract_first, preferred_element_type=jnp.float32
        )
        grad_final = jnp.dot(grad_logit, vocab_table, preferred_element_type=jnp.float32)
        grad_in, final_part = norm_back(grad_final, normed, scale_inv, final_gain)
        grad_top = grad_in.astype(jnp.bfloat16).reshape(micro_count, row_count, features)
        return (embed_head, grad_top, final_part)

    def no_head(finals):
        return (
            jnp.zeros((vocab_rows, features), jnp.float32),
            zeros_stash,
            jnp.zeros((features,), jnp.float32),
        )

    embed_head, grad_top, final_part = lax.cond(
        is_last, head, no_head, output_list.reshape(-1, features)
    )

    def backward_tick(carried, tick_index):
        arrived = carried[0]
        buffers = carried[1:]
        offset = tick_index - (sections - 1 - position)
        active = (offset >= 0) & (offset < micro_count)
        slot_index = jnp.clip(offset, 0, micro_count - 1)
        grad_out = jnp.where(is_last, pick_slot(grad_top, slot_index), arrived)

        def backward_compute(kept_activations):
            preactivation_gradients, first_row_gradients, gain_accumulated = kept_activations
            grad_float = grad_out.astype(jnp.float32)
            grad_pre = (grad_float * gelu_slope(pick_slot(preactivation_list, slot_index))).astype(
                jnp.bfloat16
            )
            grad_norm = lax.dot_general(
                grad_pre, weight, contract_last, preferred_element_type=jnp.float32
            )
            normed, scale_inv, rounded = normalize(pick_slot(input_list, slot_index), gain_row)
            grad_in, gain_part = norm_back(grad_norm, normed, scale_inv, gain_row)
            sent_output = (grad_float + grad_in).astype(jnp.bfloat16)
            kept_activations = (
                place_slot(preactivation_gradients, grad_pre, slot_index),
                place_slot(first_row_gradients, sent_output, slot_index),
                gain_accumulated + gain_part,
            )
            return (kept_activations, sent_output)

        def backward_bypass(kept_activations):
            return (kept_activations, empty_rows)

        buffers, sent_output = lax.cond(active, backward_compute, backward_bypass, buffers)
        arrived = passed_along(sent_output, "section", -1)
        return ((arrived,) + buffers, None)

    back_state = (empty_rows, zeros_stash, zeros_stash, jnp.zeros((features,), jnp.float32))
    back_final, unused_back = lax.scan(
        backward_tick, back_state, jnp.arange(tick_count, dtype=jnp.int32)
    )
    preactivation_gradients, first_row_gradients, gain_accumulated = back_final[1:]
    pres_flat = preactivation_gradients.reshape(-1, features)
    rounded_flat = rounded_list.reshape(-1, features)
    weight_part = lax.psum_scatter(
        lax.dot_general(
            rounded_flat, pres_flat, contract_first, preferred_element_type=jnp.float32
        ).astype(jnp.bfloat16),
        ("rep", "sub"),
        scatter_dimension=0,
        tiled=True,
    ).astype(jnp.float32)
    gain_total = lax.psum(gain_accumulated, ("rep", "sub"))
    final_total = lax.psum(final_part, ("section", "rep", "sub"))
    embed_in = lax.dot_general(
        onehot_in,
        first_row_gradients.reshape(-1, features),
        contract_first,
        preferred_element_type=jnp.float32,
    )
    contribution = jnp.where(is_first, embed_in, 0.0) + embed_head
    embed_total = lax.psum_scatter(
        contribution, ("section", "rep", "sub"), scatter_dimension=0, tiled=True
    )
    return (weight_part[None], gain_total[None], embed_total, final_total)


row_step = 16


def add_rows(target, other, columns=None):
    @pl.loop(0, target.shape[0] // row_step)
    def _(step):
        rows = pl.ds(pl.multiple_of(step * row_step, row_step), row_step)
        extra = other[rows, :] if columns is None else other[rows, columns]
        target[rows, :] = (target[rows, :].astype(jnp.float32) + extra.astype(jnp.float32)).astype(
            target.dtype
        )


def scatter_kernel(
    reps, weight_ref, embed_ref, small_ref, weight_out, embed_out, small_out, *scratch
):
    position, rep, sub = (lax.axis_index(name) for name in ("section", "rep", "sub"))
    chip, core = sub // 2, sub % 2
    partner = {"section": position, "rep": rep, "sub": chip * 2 + 1 - core}
    across_y = {"section": 1 - position, "rep": rep, "sub": sub}
    across_x = {"section": position, "rep": rep, "sub": (1 - chip) * 2 + core}
    up = {"section": position, "rep": lax.rem(rep + 1, reps), "sub": sub}
    down = {"section": position, "rep": lax.rem(rep + reps - 1, reps), "sub": sub}
    small_sum, small_in, send_sem, recv_sem = scratch[-4:]
    tensors = []
    for index, (source, output) in enumerate(((weight_ref, weight_out), (embed_ref, embed_out))):
        tensors.append((source, output) + tuple(scratch[7 * index : 7 * index + 7]))

    barrier = pltpu.get_barrier_semaphore()
    others = [partner, across_y, across_x] + [
        {"section": position, "rep": lax.rem(rep + hop, reps), "sub": sub}
        for hop in range(1, reps)
    ]
    for other in others:
        pl.semaphore_signal(barrier, inc=1, device_id=other, device_id_type=pl.DeviceIdType.MESH)
    pl.semaphore_wait(barrier, len(others))

    counter = [0]

    def message(source, target, device):
        number = counter[0]
        counter[0] += 1
        return pltpu.make_async_remote_copy(
            src_ref=source,
            dst_ref=target,
            send_sem=send_sem.at[number],
            recv_sem=recv_sem.at[number],
            device_id=device,
            device_id_type=pl.DeviceIdType.MESH,
        )

    pending = []

    def launch(copy):
        copy.start()
        pending.append(copy)
        return copy

    rep_order = []
    for near in range((reps + 1) // 2):
        for far in (reps - 1 - near, near):
            if far not in rep_order:
                rep_order.append(far)
    kinds = ((1, 1), (1, 0), (0, 1), (0, 0))

    def towards(flip, own):
        return 1 - own if flip else own

    small_sum[0] = small_ref[...]
    small_copies = [launch(message(small_sum.at[0], small_in.at[0], partner))]

    core_copies = {}
    for flip_s, flip_x in kinds:
        for r in rep_order:
            for t, tensor in enumerate(tensors):
                s, x = towards(flip_s, position), towards(flip_x, chip)
                core_copies[flip_s, flip_x, r, t] = launch(
                    message(tensor[0].at[s, r, x, 1 - core], tensor[2].at[s, r, x], partner)
                )
    first_a, first_b = {}, {}
    for flip_s, flip_x in kinds:
        s, x = towards(flip_s, position), towards(flip_x, chip)
        for r in rep_order:
            for t, tensor in enumerate(tensors):
                source, output, held, y_a, x_a, x_b, y_b = tensor[:7]
                core_copies[flip_s, flip_x, r, t].wait_recv()
                add_rows(held.at[s, r, x], source.at[s, r, x, core])
                half = held.shape[-1] // 2
                if flip_s:
                    first_a[flip_x, r, t] = launch(
                        message(held.at[s, r, x, :, pl.ds(0, half)], y_a.at[x, r], across_y)
                    )
                if flip_x:
                    first_b[flip_s, r, t] = launch(
                        message(held.at[s, r, x, :, pl.ds(half, half)], x_b.at[s, r], across_x)
                    )
    small_copies[0].wait_recv()
    small_sum[1] = small_sum[0] + small_in[0]
    small_copies.append(launch(message(small_sum.at[1], small_in.at[1], across_y)))

    second_a, second_b = {}, {}
    for flip in (1, 0):
        for r in rep_order:
            for t, tensor in enumerate(tensors):
                source, output, held, y_a, x_a, x_b, y_b = tensor[:7]
                half = held.shape[-1] // 2
                x = towards(flip, chip)
                first_a[flip, r, t].wait_recv()
                add_rows(y_a.at[x, r], held.at[position, r, x], pl.ds(0, half))
                s = towards(flip, position)
                first_b[flip, r, t].wait_recv()
                add_rows(x_b.at[s, r], held.at[s, r, chip], pl.ds(half, half))
                if flip:
                    second_a[r, t] = launch(message(y_a.at[x, r], x_a.at[r], across_x))
                    second_b[r, t] = launch(message(x_b.at[s, r], y_b.at[r], across_y))
    small_copies[1].wait_recv()
    small_sum[2] = small_sum[1] + small_in[1]
    small_copies.append(launch(message(small_sum.at[2], small_in.at[2], across_x)))

    for r in rep_order:
        for t, tensor in enumerate(tensors):
            source, output, held, y_a, x_a, x_b, y_b = tensor[:7]
            second_a[r, t].wait_recv()
            add_rows(x_a.at[r], y_a.at[chip, r])
            second_b[r, t].wait_recv()
            add_rows(y_b.at[r], x_b.at[position, r])
    small_copies[2].wait_recv()
    small_sum[3] = small_sum[2] + small_in[2]
    small_gather = []
    for hop in range(1, reps):
        there = {"section": position, "rep": lax.rem(rep + hop, reps), "sub": sub}
        small_gather.append(launch(message(small_sum.at[3], small_in.at[2 + hop], there)))

    ends = []
    for step in range(reps - 1):
        for t, tensor in enumerate(tensors):
            x_a, y_b = tensor[4], tensor[6]
            z_up, z_down = tensor[7:9]
            for color, own in enumerate((x_a, y_b)):
                for buffer, target, device, upward in (
                    (z_up, reps - 1 - step, up, True),
                    (z_down, step, down, False),
                ):
                    at_start = rep == (0 if upward else reps - 1)
                    passes = rep < target if upward else rep > target
                    here = buffer.at[color, target]
                    fresh = message(own.at[target], here, device)
                    counter[0] -= 1
                    passed = message(here, here, device)

                    @pl.when(jnp.logical_and(jnp.logical_not(at_start), jnp.logical_or(passes, rep == target)))
                    def _():
                        passed.wait_recv()

                    @pl.when(jnp.logical_and(jnp.logical_not(at_start), passes))
                    def _():
                        add_rows(here, own.at[target])
                        passed.start()

                    @pl.when(jnp.logical_and(at_start, passes))
                    def _():
                        fresh.start()

                    ends.append((passes, passed))
    for t, tensor in enumerate(tensors):
        output, x_a, y_b = tensor[1], tensor[4], tensor[6]
        z_up, z_down = tensor[7:9]
        half = x_a.shape[-1]
        for color, own in enumerate((x_a, y_b)):

            @pl.loop(0, own.shape[1] // row_step)
            def _(step):
                rows = pl.ds(pl.multiple_of(step * row_step, row_step), row_step)
                output[rows, pl.ds(color * half, half)] = own[rep, rows, :].astype(jnp.float32)

            for buffer, edge in ((z_up, 0), (z_down, reps - 1)):

                @pl.when(rep != edge)
                def _():
                    @pl.loop(0, own.shape[1] // row_step)
                    def _(step):
                        rows = pl.ds(pl.multiple_of(step * row_step, row_step), row_step)
                        output[rows, pl.ds(color * half, half)] += buffer[color, rep, rows, :].astype(
                            jnp.float32
                        )

    for copy in small_gather:
        copy.wait_recv()
    total = small_sum[3]
    for hop in range(1, reps):
        total = total + small_in[2 + hop]
    small_out[...] = total
    for copy in pending:
        copy.wait_send()
    for passes, copy in ends:

        @pl.when(passes)
        def _():
            copy.wait_send()


def scatter_sums(weight_part, embed_part, small_part):
    sections, reps, subs = (lax.axis_size(name) for name in ("section", "rep", "sub"))
    devices = sections * reps * subs
    kinds = (sections, reps, subs // 2, 2)
    weight_rows = weight_part.shape[0] // devices
    columns = weight_part.shape[1]
    embed_rows = embed_part.shape[0] // devices
    fold = max(1, row_step // embed_rows)
    weight_in = weight_part.reshape(kinds + (weight_rows, columns))
    embed_in = embed_part.astype(jnp.bfloat16).reshape(
        kinds + (embed_rows * fold, columns // fold)
    )
    pad = (-small_part.shape[0]) % 8
    small_in = jnp.pad(small_part, ((0, pad), (0, 0)))
    scratch = []
    for rows, width in (weight_in.shape[-2:], embed_in.shape[-2:]):
        half = width // 2
        for lead in (
            (sections, reps, subs // 2, rows, width),
            (subs // 2, reps, rows, half),
            (reps, rows, half),
            (sections, reps, rows, half),
            (reps, rows, half),
            (2, reps, rows, half),
            (2, reps, rows, half),
        ):
            scratch.append(pltpu.VMEM(lead, jnp.bfloat16))
    messages = 2 * (4 * reps + 4 * reps + 2 * reps + 4 * (reps - 1)) + 2 * 4 * reps + 3 + reps
    scratch += [
        pltpu.VMEM((4,) + small_in.shape, jnp.float32),
        pltpu.VMEM((2 + reps,) + small_in.shape, jnp.float32),
        pltpu.SemaphoreType.DMA((messages,)),
        pltpu.SemaphoreType.DMA((messages,)),
    ]
    vmem = pl.BlockSpec(memory_space=pltpu.VMEM)
    weight_sum, embed_sum, small_sum = pl.pallas_call(
        functools.partial(scatter_kernel, reps),
        out_shape=(
            jax.ShapeDtypeStruct(weight_in.shape[-2:], jnp.float32),
            jax.ShapeDtypeStruct(embed_in.shape[-2:], jnp.float32),
            jax.ShapeDtypeStruct(small_in.shape, jnp.float32),
        ),
        in_specs=[vmem] * 3,
        out_specs=(vmem,) * 3,
        scratch_shapes=scratch,
        compiler_params=pltpu.CompilerParams(
            collective_id=1, has_side_effects=True, vmem_limit_bytes=60 * 1024 * 1024
        ),
        name="scatter_sums",
    )(weight_in, embed_in, small_in)
    return weight_sum, embed_sum.reshape(embed_rows, columns), small_sum[: small_part.shape[0]]


def fits_replicated(mesh, weight_shape):
    layers, rows, columns = weight_shape
    return layers * rows * columns * 2 <= 16 * 1024 * 1024


def replicated_body(token_ids, target_ids, embedding, section_weight, section_gain, final_gain):
    axes = ("section", "rep", "sub")
    sections = lax.axis_size("section")
    position = lax.axis_index("section")
    features = embedding.shape[1]
    vocab_rows = embedding.shape[0] * lax.axis_size(("rep", "sub"))
    token_count = token_ids.size // sections
    contract_last = (((1,), (1,)), ((), ()))
    contract_first = (((0,), (0,)), ((), ()))
    vocab_table = lax.all_gather(embedding, ("rep", "sub"), axis=0, tiled=True)
    weights = lax.all_gather(section_weight[0], axes, axis=0, tiled=True)
    weights = weights.reshape(sections, features, features)
    gains = lax.all_gather(section_gain, "section", axis=0, tiled=True)
    my_tokens = lax.dynamic_slice_in_dim(token_ids.reshape(-1), position * token_count, token_count)
    my_targets = lax.dynamic_slice_in_dim(target_ids.reshape(-1), position * token_count, token_count)
    vocab_iota = jnp.arange(vocab_rows, dtype=jnp.int32)
    onehot_in = (my_tokens[:, None] == vocab_iota[None, :]).astype(jnp.bfloat16)
    residual = jnp.dot(onehot_in, vocab_table, preferred_element_type=jnp.float32).astype(
        jnp.bfloat16
    )
    saved = []
    for layer in range(sections):
        normed, scale_inv, rounded = normalize(residual, gains[layer])
        pre_act = jnp.dot(rounded, weights[layer], preferred_element_type=jnp.float32)
        saved.append((normed, scale_inv, rounded, pre_act))
        residual = (residual.astype(jnp.float32) + gelu(pre_act)).astype(jnp.bfloat16)
    logit_scale = float(features) ** (-0.5)
    normed, scale_inv, final_rows = normalize(residual, final_gain)
    logits = (
        lax.dot_general(final_rows, vocab_table, contract_last, preferred_element_type=jnp.float32)
        * logit_scale
    )
    exp_logit = jnp.exp(logits)
    probability = exp_logit / jnp.sum(exp_logit, axis=-1, keepdims=True)
    onehot_out = (my_targets[:, None] == vocab_iota[None, :]).astype(jnp.float32)
    grad_logit = ((probability - onehot_out) * logit_scale).astype(jnp.bfloat16)
    embed_head = lax.dot_general(
        grad_logit, final_rows, contract_first, preferred_element_type=jnp.float32
    )
    grad_final = jnp.dot(grad_logit, vocab_table, preferred_element_type=jnp.float32)
    grad_in, final_part = norm_back(grad_final, normed, scale_inv, final_gain)
    grad_residual = grad_in.astype(jnp.bfloat16)
    weight_parts = []
    small_parts = [final_part]
    for layer in reversed(range(sections)):
        normed, scale_inv, rounded, pre_act = saved[layer]
        grad_float = grad_residual.astype(jnp.float32)
        grad_pre = (grad_float * gelu_slope(pre_act)).astype(jnp.bfloat16)
        weight_parts.append(
            lax.dot_general(
                rounded, grad_pre, contract_first, preferred_element_type=jnp.float32
            ).astype(jnp.bfloat16)
        )
        grad_norm = lax.dot_general(
            grad_pre, weights[layer], contract_last, preferred_element_type=jnp.float32
        )
        grad_in, gain_part = norm_back(grad_norm, normed, scale_inv, gains[layer])
        small_parts.append(gain_part)
        grad_residual = (grad_float + grad_in).astype(jnp.bfloat16)
    embed_part = embed_head + lax.dot_general(
        onehot_in, grad_residual, contract_first, preferred_element_type=jnp.float32
    )
    return finish(weight_parts[::-1], embed_part, jnp.stack(small_parts), axes, position, sections)


def finish(weight_parts, embed_part, small_part, axes, position, sections):
    weight_all = jnp.concatenate(weight_parts, axis=0)
    if sections == 2 and lax.axis_size("sub") == 4 and lax.axis_size("rep") > 1:
        weight_total, embed_total, small_total = scatter_sums(weight_all, embed_part, small_part)
        gain_total = lax.dynamic_slice_in_dim(small_total, sections - position, 1, axis=0)
        return (weight_total[None], gain_total, embed_total, small_total[0])
    weight_total = lax.psum_scatter(weight_all, axes, scatter_dimension=0, tiled=True)
    embed_total = lax.psum_scatter(embed_part, axes, scatter_dimension=0, tiled=True)
    small_total = lax.psum(small_part, axes)
    gain_total = lax.dynamic_slice_in_dim(small_total, sections - position, 1, axis=0)
    return (weight_total.astype(jnp.float32)[None], gain_total, embed_total, small_total[0])


def solution(mesh):
    in_specs = (
        P(None, ("rep", "sub")),
        P(None, ("rep", "sub")),
        P(("rep", "sub"), None),
        P("section", ("rep", "sub"), None),
        P("section", None),
        P(),
    )
    out_specs = (
        P("section", ("rep", "sub"), None),
        P("section", None),
        P(("section", "rep", "sub"), None),
        P(),
    )

    def step(*arguments):
        tokens = arguments[0].size // (mesh.shape["rep"] * mesh.shape["sub"])
        replicated = fits_replicated(mesh, arguments[3].shape) and tokens % mesh.shape["section"] == 0
        chosen = replicated_body if replicated else pipeline_body
        return jax.shard_map(
            chosen, mesh=mesh, in_specs=in_specs, out_specs=out_specs, check_vma=False
        )(*arguments)

    return step
```

```python
import functools
import jax
import jax.numpy as jnp
from jax import lax
from jax.experimental import pallas as pl
from jax.experimental.pallas import tpu as pltpu
from jax.sharding import PartitionSpec as P

epsilon = 1e-06
gelu_coef = 0.7978845608028654
cube_coef = 0.044715


def passed_along(value, axis, steps):
    count = lax.axis_size(axis)
    initial, last = (max(0, -steps), min(count, count - steps))
    return lax.ppermute(value, axis, [(source, source + steps) for source in range(initial, last)])


def gelu(pre_act):
    return (
        0.5
        * pre_act
        * (1.0 + jnp.tanh(gelu_coef * (pre_act + cube_coef * pre_act * pre_act * pre_act)))
    )


def gelu_slope(pre_act):
    inside = gelu_coef * (pre_act + cube_coef * pre_act * pre_act * pre_act)
    tangent = jnp.tanh(inside)
    return 0.5 * (1.0 + tangent) + 0.5 * pre_act * (1.0 - tangent * tangent) * gelu_coef * (
        1.0 + 3.0 * cube_coef * pre_act * pre_act
    )


def normalize(residual, gain_row):
    values = residual.astype(jnp.float32)
    scale_inv = lax.rsqrt(jnp.mean(values * values, axis=-1, keepdims=True) + epsilon)
    normed = values * scale_inv
    return (normed, scale_inv, (normed * gain_row).astype(jnp.bfloat16))


def norm_back(grad_norm, normed, scale_inv, gain_row):
    grad_unit = grad_norm * gain_row
    grad_in = scale_inv * (
        grad_unit - normed * jnp.mean(grad_unit * normed, axis=-1, keepdims=True)
    )
    return (grad_in, jnp.sum(grad_norm * normed, axis=0))


def pick_slot(buffer, slot_index):
    return lax.dynamic_index_in_dim(buffer, slot_index, 0, keepdims=False)


def place_slot(buffer, update, slot_index):
    return lax.dynamic_update_index_in_dim(buffer, update, slot_index, 0)


def pipeline_body(token_ids, target_ids, embedding, section_weight, section_gain, final_gain):
    sections = lax.axis_size("section")
    position = lax.axis_index("section")
    micro_count = token_ids.shape[0]
    row_count = token_ids.shape[1]
    features = embedding.shape[1]
    group_size = lax.axis_size(("rep", "sub"))
    vocab_rows = embedding.shape[0] * group_size
    tick_count = micro_count + sections - 1
    contract_last = (((1,), (1,)), ((), ()))
    contract_first = (((0,), (0,)), ((), ()))
    vocab_table = lax.all_gather(embedding, ("rep", "sub"), axis=0, tiled=True)
    weight = lax.all_gather(section_weight, ("rep", "sub"), axis=1, tiled=True)[0]
    gain_row = section_gain[0]
    is_first = position == 0
    is_last = position == sections - 1
    vocab_iota = jnp.arange(vocab_rows, dtype=jnp.int32)
    onehot_in = (token_ids.reshape(-1)[:, None] == vocab_iota[None, :]).astype(jnp.bfloat16)
    embedded = jnp.dot(onehot_in, vocab_table, preferred_element_type=jnp.float32).astype(
        jnp.bfloat16
    )
    embedded = embedded.reshape(micro_count, row_count, features)
    empty_rows = jnp.zeros((row_count, features), jnp.bfloat16)
    zeros_stash = jnp.zeros((micro_count, row_count, features), jnp.bfloat16)
    zeros_pre = jnp.zeros((micro_count, row_count, features), jnp.float32)

    def forward_tick(carried, tick_index):
        arrived = carried[0]
        buffers = carried[1:]
        offset = tick_index - position
        active = (offset >= 0) & (offset < micro_count)
        slot_index = jnp.clip(offset, 0, micro_count - 1)
        residual = jnp.where(is_first, pick_slot(embedded, slot_index), arrived)

        def forward_compute(kept_activations):
            input_list, rounded_list, preactivation_list, output_list = kept_activations
            normed, scale_inv, rounded = normalize(residual, gain_row)
            pre_act = jnp.dot(rounded, weight, preferred_element_type=jnp.float32)
            returned_value = (residual.astype(jnp.float32) + gelu(pre_act)).astype(jnp.bfloat16)
            kept_activations = (
                place_slot(input_list, residual, slot_index),
                place_slot(rounded_list, rounded, slot_index),
                place_slot(preactivation_list, pre_act, slot_index),
                place_slot(output_list, returned_value, slot_index),
            )
            return (kept_activations, returned_value)

        def forward_bypass(kept_activations):
            return (kept_activations, empty_rows)

        buffers, returned_value = lax.cond(active, forward_compute, forward_bypass, buffers)
        arrived = passed_along(returned_value, "section", 1)
        return ((arrived,) + buffers, None)

    start_state = (empty_rows, zeros_stash, zeros_stash, zeros_pre, zeros_stash)
    final_state, unused_out = lax.scan(
        forward_tick, start_state, jnp.arange(tick_count, dtype=jnp.int32)
    )
    input_list, rounded_list, preactivation_list, output_list = final_state[1:]
    logit_scale = float(features) ** (-0.5)

    def head(finals):
        normed, scale_inv, final_rows = normalize(finals, final_gain)
        logits = (
            lax.dot_general(
                final_rows, vocab_table, contract_last, preferred_element_type=jnp.float32
            )
            * logit_scale
        )
        exp_logit = jnp.exp(logits)
        probability = exp_logit / jnp.sum(exp_logit, axis=-1, keepdims=True)
        onehot_out = (target_ids.reshape(-1)[:, None] == vocab_iota[None, :]).astype(jnp.float32)
        grad_logit = ((probability - onehot_out) * logit_scale).astype(jnp.bfloat16)
        embed_head = lax.dot_general(
            grad_logit, final_rows, contract_first, preferred_element_type=jnp.float32
        )
        grad_final = jnp.dot(grad_logit, vocab_table, preferred_element_type=jnp.float32)
        grad_in, final_part = norm_back(grad_final, normed, scale_inv, final_gain)
        grad_top = grad_in.astype(jnp.bfloat16).reshape(micro_count, row_count, features)
        return (embed_head, grad_top, final_part)

    def no_head(finals):
        return (
            jnp.zeros((vocab_rows, features), jnp.float32),
            zeros_stash,
            jnp.zeros((features,), jnp.float32),
        )

    embed_head, grad_top, final_part = lax.cond(
        is_last, head, no_head, output_list.reshape(-1, features)
    )

    def backward_tick(carried, tick_index):
        arrived = carried[0]
        buffers = carried[1:]
        offset = tick_index - (sections - 1 - position)
        active = (offset >= 0) & (offset < micro_count)
        slot_index = jnp.clip(offset, 0, micro_count - 1)
        grad_out = jnp.where(is_last, pick_slot(grad_top, slot_index), arrived)

        def backward_compute(kept_activations):
            preactivation_gradients, first_row_gradients, gain_accumulated = kept_activations
            grad_float = grad_out.astype(jnp.float32)
            grad_pre = (grad_float * gelu_slope(pick_slot(preactivation_list, slot_index))).astype(
                jnp.bfloat16
            )
            grad_norm = lax.dot_general(
                grad_pre, weight, contract_last, preferred_element_type=jnp.float32
            )
            normed, scale_inv, rounded = normalize(pick_slot(input_list, slot_index), gain_row)
            grad_in, gain_part = norm_back(grad_norm, normed, scale_inv, gain_row)
            sent_output = (grad_float + grad_in).astype(jnp.bfloat16)
            kept_activations = (
                place_slot(preactivation_gradients, grad_pre, slot_index),
                place_slot(first_row_gradients, sent_output, slot_index),
                gain_accumulated + gain_part,
            )
            return (kept_activations, sent_output)

        def backward_bypass(kept_activations):
            return (kept_activations, empty_rows)

        buffers, sent_output = lax.cond(active, backward_compute, backward_bypass, buffers)
        arrived = passed_along(sent_output, "section", -1)
        return ((arrived,) + buffers, None)

    back_state = (empty_rows, zeros_stash, zeros_stash, jnp.zeros((features,), jnp.float32))
    back_final, unused_back = lax.scan(
        backward_tick, back_state, jnp.arange(tick_count, dtype=jnp.int32)
    )
    preactivation_gradients, first_row_gradients, gain_accumulated = back_final[1:]
    pres_flat = preactivation_gradients.reshape(-1, features)
    rounded_flat = rounded_list.reshape(-1, features)
    weight_part = lax.psum_scatter(
        lax.dot_general(
            rounded_flat, pres_flat, contract_first, preferred_element_type=jnp.float32
        ).astype(jnp.bfloat16),
        ("rep", "sub"),
        scatter_dimension=0,
        tiled=True,
    ).astype(jnp.float32)
    gain_total = lax.psum(gain_accumulated, ("rep", "sub"))
    final_total = lax.psum(final_part, ("section", "rep", "sub"))
    embed_in = lax.dot_general(
        onehot_in,
        first_row_gradients.reshape(-1, features),
        contract_first,
        preferred_element_type=jnp.float32,
    )
    contribution = jnp.where(is_first, embed_in, 0.0) + embed_head
    embed_total = lax.psum_scatter(
        contribution, ("section", "rep", "sub"), scatter_dimension=0, tiled=True
    )
    return (weight_part[None], gain_total[None], embed_total, final_total)


row_step = 16


def add_rows(target, other, columns=None):
    @pl.loop(0, target.shape[0] // row_step)
    def _(step):
        rows = pl.ds(pl.multiple_of(step * row_step, row_step), row_step)
        extra = other[rows, :] if columns is None else other[rows, columns]
        target[rows, :] = (target[rows, :].astype(jnp.float32) + extra.astype(jnp.float32)).astype(
            target.dtype
        )


def scatter_kernel(
    reps, weight_ref, embed_ref, small_ref, weight_out, embed_out, small_out, *scratch
):
    position, rep, sub = (lax.axis_index(name) for name in ("section", "rep", "sub"))
    chip, core = sub // 2, sub % 2
    partner = {"section": position, "rep": rep, "sub": chip * 2 + 1 - core}
    across_y = {"section": 1 - position, "rep": rep, "sub": sub}
    across_x = {"section": position, "rep": rep, "sub": (1 - chip) * 2 + core}
    up = {"section": position, "rep": lax.rem(rep + 1, reps), "sub": sub}
    down = {"section": position, "rep": lax.rem(rep + reps - 1, reps), "sub": sub}
    small_sum, small_in, send_sem, recv_sem = scratch[-4:]
    tensors = []
    for index, (source, output) in enumerate(((weight_ref, weight_out), (embed_ref, embed_out))):
        tensors.append((source, output) + tuple(scratch[7 * index : 7 * index + 7]))

    barrier = pltpu.get_barrier_semaphore()
    others = [partner, across_y, across_x] + [
        {"section": position, "rep": lax.rem(rep + hop, reps), "sub": sub}
        for hop in range(1, reps)
    ]
    for other in others:
        pl.semaphore_signal(barrier, inc=1, device_id=other, device_id_type=pl.DeviceIdType.MESH)
    pl.semaphore_wait(barrier, len(others))

    counter = [0]

    def message(source, target, device):
        number = counter[0]
        counter[0] += 1
        return pltpu.make_async_remote_copy(
            src_ref=source,
            dst_ref=target,
            send_sem=send_sem.at[number],
            recv_sem=recv_sem.at[number],
            device_id=device,
            device_id_type=pl.DeviceIdType.MESH,
        )

    pending = []

    def launch(copy):
        copy.start()
        pending.append(copy)
        return copy

    rep_order = []
    for near in range((reps + 1) // 2):
        for far in (reps - 1 - near, near):
            if far not in rep_order:
                rep_order.append(far)
    kinds = ((1, 1), (1, 0), (0, 1), (0, 0))

    def towards(flip, own):
        return 1 - own if flip else own

    small_sum[0] = small_ref[...]
    small_copies = [launch(message(small_sum.at[0], small_in.at[0], partner))]

    core_copies = {}
    for flip_s, flip_x in kinds:
        for r in rep_order:
            for t, tensor in enumerate(tensors):
                s, x = towards(flip_s, position), towards(flip_x, chip)
                core_copies[flip_s, flip_x, r, t] = launch(
                    message(tensor[0].at[s, r, x, 1 - core], tensor[2].at[s, r, x], partner)
                )
    first_a, first_b = {}, {}
    for flip_s, flip_x in kinds:
        s, x = towards(flip_s, position), towards(flip_x, chip)
        for r in rep_order:
            for t, tensor in enumerate(tensors):
                source, output, held, y_a, x_a, x_b, y_b = tensor[:7]
                core_copies[flip_s, flip_x, r, t].wait_recv()
                add_rows(held.at[s, r, x], source.at[s, r, x, core])
                half = held.shape[-1] // 2
                if flip_s:
                    first_a[flip_x, r, t] = launch(
                        message(held.at[s, r, x, :, pl.ds(0, half)], y_a.at[x, r], across_y)
                    )
                if flip_x:
                    first_b[flip_s, r, t] = launch(
                        message(held.at[s, r, x, :, pl.ds(half, half)], x_b.at[s, r], across_x)
                    )
    small_copies[0].wait_recv()
    small_sum[1] = small_sum[0] + small_in[0]
    small_copies.append(launch(message(small_sum.at[1], small_in.at[1], across_y)))

    second_a, second_b = {}, {}
    for flip in (1, 0):
        for r in rep_order:
            for t, tensor in enumerate(tensors):
                source, output, held, y_a, x_a, x_b, y_b = tensor[:7]
                half = held.shape[-1] // 2
                x = towards(flip, chip)
                first_a[flip, r, t].wait_recv()
                add_rows(y_a.at[x, r], held.at[position, r, x], pl.ds(0, half))
                s = towards(flip, position)
                first_b[flip, r, t].wait_recv()
                add_rows(x_b.at[s, r], held.at[s, r, chip], pl.ds(half, half))
                if flip:
                    second_a[r, t] = launch(message(y_a.at[x, r], x_a.at[r], across_x))
                    second_b[r, t] = launch(message(x_b.at[s, r], y_b.at[r], across_y))
    small_copies[1].wait_recv()
    small_sum[2] = small_sum[1] + small_in[1]
    small_copies.append(launch(message(small_sum.at[2], small_in.at[2], across_x)))

    for r in rep_order:
        for t, tensor in enumerate(tensors):
            source, output, held, y_a, x_a, x_b, y_b = tensor[:7]
            second_a[r, t].wait_recv()
            add_rows(x_a.at[r], y_a.at[chip, r])
            second_b[r, t].wait_recv()
            add_rows(y_b.at[r], x_b.at[position, r])
    small_copies[2].wait_recv()
    small_sum[3] = small_sum[2] + small_in[2]
    small_gather = []
    for hop in range(1, reps):
        there = {"section": position, "rep": lax.rem(rep + hop, reps), "sub": sub}
        small_gather.append(launch(message(small_sum.at[3], small_in.at[2 + hop], there)))

    ends = []
    for step in range(reps - 1):
        for t, tensor in enumerate(tensors):
            x_a, y_b = tensor[4], tensor[6]
            z_up, z_down = tensor[7:9]
            for color, own in enumerate((x_a, y_b)):
                for buffer, target, device, upward in (
                    (z_up, reps - 1 - step, up, True),
                    (z_down, step, down, False),
                ):
                    at_start = rep == (0 if upward else reps - 1)
                    passes = rep < target if upward else rep > target
                    here = buffer.at[color, target]
                    fresh = message(own.at[target], here, device)
                    counter[0] -= 1
                    passed = message(here, here, device)

                    @pl.when(jnp.logical_and(jnp.logical_not(at_start), jnp.logical_or(passes, rep == target)))
                    def _():
                        passed.wait_recv()

                    @pl.when(jnp.logical_and(jnp.logical_not(at_start), passes))
                    def _():
                        add_rows(here, own.at[target])
                        passed.start()

                    @pl.when(jnp.logical_and(at_start, passes))
                    def _():
                        fresh.start()

                    ends.append((passes, passed))
    for t, tensor in enumerate(tensors):
        output, x_a, y_b = tensor[1], tensor[4], tensor[6]
        z_up, z_down = tensor[7:9]
        half = x_a.shape[-1]
        for color, own in enumerate((x_a, y_b)):

            @pl.loop(0, own.shape[1] // row_step)
            def _(step):
                rows = pl.ds(pl.multiple_of(step * row_step, row_step), row_step)
                output[rows, pl.ds(color * half, half)] = own[rep, rows, :].astype(jnp.float32)

            for buffer, edge in ((z_up, 0), (z_down, reps - 1)):

                @pl.when(rep != edge)
                def _():
                    @pl.loop(0, own.shape[1] // row_step)
                    def _(step):
                        rows = pl.ds(pl.multiple_of(step * row_step, row_step), row_step)
                        output[rows, pl.ds(color * half, half)] += buffer[color, rep, rows, :].astype(
                            jnp.float32
                        )

    for copy in small_gather:
        copy.wait_recv()
    total = small_sum[3]
    for hop in range(1, reps):
        total = total + small_in[2 + hop]
    small_out[...] = total
    for copy in pending:
        copy.wait_send()
    for passes, copy in ends:

        @pl.when(passes)
        def _():
            copy.wait_send()


def scatter_sums(weight_part, embed_part, small_part):
    sections, reps, subs = (lax.axis_size(name) for name in ("section", "rep", "sub"))
    devices = sections * reps * subs
    kinds = (sections, reps, subs // 2, 2)
    weight_rows = weight_part.shape[0] // devices
    columns = weight_part.shape[1]
    embed_rows = embed_part.shape[0] // devices
    fold = max(1, row_step // embed_rows)
    weight_in = weight_part.reshape(kinds + (weight_rows, columns))
    embed_in = embed_part.astype(jnp.bfloat16).reshape(
        kinds + (embed_rows * fold, columns // fold)
    )
    pad = (-small_part.shape[0]) % 8
    small_in = jnp.pad(small_part, ((0, pad), (0, 0)))
    scratch = []
    for rows, width in (weight_in.shape[-2:], embed_in.shape[-2:]):
        half = width // 2
        for lead in (
            (sections, reps, subs // 2, rows, width),
            (subs // 2, reps, rows, half),
            (reps, rows, half),
            (sections, reps, rows, half),
            (reps, rows, half),
            (2, reps, rows, half),
            (2, reps, rows, half),
        ):
            scratch.append(pltpu.VMEM(lead, jnp.bfloat16))
    messages = 2 * (4 * reps + 4 * reps + 2 * reps + 4 * (reps - 1)) + 2 * 4 * reps + 3 + reps
    scratch += [
        pltpu.VMEM((4,) + small_in.shape, jnp.float32),
        pltpu.VMEM((2 + reps,) + small_in.shape, jnp.float32),
        pltpu.SemaphoreType.DMA((messages,)),
        pltpu.SemaphoreType.DMA((messages,)),
    ]
    vmem = pl.BlockSpec(memory_space=pltpu.VMEM)
    weight_sum, embed_sum, small_sum = pl.pallas_call(
        functools.partial(scatter_kernel, reps),
        out_shape=(
            jax.ShapeDtypeStruct(weight_in.shape[-2:], jnp.float32),
            jax.ShapeDtypeStruct(embed_in.shape[-2:], jnp.float32),
            jax.ShapeDtypeStruct(small_in.shape, jnp.float32),
        ),
        in_specs=[vmem] * 3,
        out_specs=(vmem,) * 3,
        scratch_shapes=scratch,
        compiler_params=pltpu.CompilerParams(
            collective_id=1, has_side_effects=True, vmem_limit_bytes=60 * 1024 * 1024
        ),
        name="scatter_sums",
    )(weight_in, embed_in, small_in)
    return weight_sum, embed_sum.reshape(embed_rows, columns), small_sum[: small_part.shape[0]]


def fits_replicated(mesh, weight_shape):
    layers, rows, columns = weight_shape
    return layers * rows * columns * 2 <= 16 * 1024 * 1024


def replicated_body(token_ids, target_ids, embedding, section_weight, section_gain, final_gain):
    axes = ("section", "rep", "sub")
    sections = lax.axis_size("section")
    position = lax.axis_index("section")
    features = embedding.shape[1]
    vocab_rows = embedding.shape[0] * lax.axis_size(("rep", "sub"))
    token_count = token_ids.size // sections
    contract_last = (((1,), (1,)), ((), ()))
    contract_first = (((0,), (0,)), ((), ()))
    half = features // 2
    vocab_table = jnp.concatenate(
        [
            lax.all_gather(part, ("rep", "sub"), axis=0, tiled=True)
            for part in (embedding[:, :half], embedding[:, half:])
        ],
        axis=1,
    )
    weights = lax.all_gather(section_weight[0], axes, axis=0, tiled=True)
    weights = weights.reshape(sections, features, features)
    gains = lax.all_gather(section_gain, "section", axis=0, tiled=True)
    my_tokens = lax.dynamic_slice_in_dim(token_ids.reshape(-1), position * token_count, token_count)
    my_targets = lax.dynamic_slice_in_dim(target_ids.reshape(-1), position * token_count, token_count)
    vocab_iota = jnp.arange(vocab_rows, dtype=jnp.int32)
    onehot_in = (my_tokens[:, None] == vocab_iota[None, :]).astype(jnp.bfloat16)
    residual = jnp.dot(onehot_in, vocab_table, preferred_element_type=jnp.float32).astype(
        jnp.bfloat16
    )
    saved = []
    for layer in range(sections):
        normed, scale_inv, rounded = normalize(residual, gains[layer])
        pre_act = jnp.dot(rounded, weights[layer], preferred_element_type=jnp.float32)
        saved.append((normed, scale_inv, rounded, pre_act))
        residual = (residual.astype(jnp.float32) + gelu(pre_act)).astype(jnp.bfloat16)
    logit_scale = float(features) ** (-0.5)
    normed, scale_inv, final_rows = normalize(residual, final_gain)
    logits = (
        lax.dot_general(final_rows, vocab_table, contract_last, preferred_element_type=jnp.float32)
        * logit_scale
    )
    exp_logit = jnp.exp(logits)
    probability = exp_logit / jnp.sum(exp_logit, axis=-1, keepdims=True)
    onehot_out = (my_targets[:, None] == vocab_iota[None, :]).astype(jnp.float32)
    grad_logit = ((probability - onehot_out) * logit_scale).astype(jnp.bfloat16)
    embed_head = lax.dot_general(
        grad_logit, final_rows, contract_first, preferred_element_type=jnp.float32
    )
    grad_final = jnp.dot(grad_logit, vocab_table, preferred_element_type=jnp.float32)
    grad_in, final_part = norm_back(grad_final, normed, scale_inv, final_gain)
    grad_residual = grad_in.astype(jnp.bfloat16)
    weight_parts = []
    small_parts = [final_part]
    for layer in reversed(range(sections)):
        normed, scale_inv, rounded, pre_act = saved[layer]
        grad_float = grad_residual.astype(jnp.float32)
        grad_pre = (grad_float * gelu_slope(pre_act)).astype(jnp.bfloat16)
        weight_parts.append(
            lax.dot_general(
                rounded, grad_pre, contract_first, preferred_element_type=jnp.float32
            ).astype(jnp.bfloat16)
        )
        grad_norm = lax.dot_general(
            grad_pre, weights[layer], contract_last, preferred_element_type=jnp.float32
        )
        grad_in, gain_part = norm_back(grad_norm, normed, scale_inv, gains[layer])
        small_parts.append(gain_part)
        grad_residual = (grad_float + grad_in).astype(jnp.bfloat16)
    embed_part = embed_head + lax.dot_general(
        onehot_in, grad_residual, contract_first, preferred_element_type=jnp.float32
    )
    return finish(weight_parts[::-1], embed_part, jnp.stack(small_parts), axes, position, sections)


def finish(weight_parts, embed_part, small_part, axes, position, sections):
    weight_all = jnp.concatenate(weight_parts, axis=0)
    if sections == 2 and lax.axis_size("sub") == 4 and lax.axis_size("rep") > 1:
        weight_total, embed_total, small_total = scatter_sums(weight_all, embed_part, small_part)
        gain_total = lax.dynamic_slice_in_dim(small_total, sections - position, 1, axis=0)
        return (weight_total[None], gain_total, embed_total, small_total[0])
    weight_total = lax.psum_scatter(weight_all, axes, scatter_dimension=0, tiled=True)
    embed_total = lax.psum_scatter(embed_part, axes, scatter_dimension=0, tiled=True)
    small_total = lax.psum(small_part, axes)
    gain_total = lax.dynamic_slice_in_dim(small_total, sections - position, 1, axis=0)
    return (weight_total.astype(jnp.float32)[None], gain_total, embed_total, small_total[0])


def solution(mesh):
    in_specs = (
        P(None, ("rep", "sub")),
        P(None, ("rep", "sub")),
        P(("rep", "sub"), None),
        P("section", ("rep", "sub"), None),
        P("section", None),
        P(),
    )
    out_specs = (
        P("section", ("rep", "sub"), None),
        P("section", None),
        P(("section", "rep", "sub"), None),
        P(),
    )

    def step(*arguments):
        tokens = arguments[0].size // (mesh.shape["rep"] * mesh.shape["sub"])
        replicated = fits_replicated(mesh, arguments[3].shape) and tokens % mesh.shape["section"] == 0
        chosen = replicated_body if replicated else pipeline_body
        return jax.shard_map(
            chosen, mesh=mesh, in_specs=in_specs, out_specs=out_specs, check_vma=False
        )(*arguments)

    return step
```
